32 devices in a mesh: row: 2 (over x), col: 4 (over z), depth: 4 (over y, core).
Axes of the slice: x: 2, y: 2, z: 4, core: 2. Of those that a mesh axis runs over, the one named last changes fastest.
Arguments:
- pair: bfloat16 [768, 768, 128], P('row', 'col'), may hold values from -6 to 6
- ln_gain: float32 [128], replicated, may hold values from 0.1 to 1.9
- ln_shift: float32 [128], replicated, may hold values from -3 to 3
- proj_weight: bfloat16 [128, 512], replicated, may hold values from -0.5 to 0.5
- proj_bias: float32 [512], replicated, may hold values from -3 to 3
- gate_weight: bfloat16 [128, 128], replicated, may hold values from -0.5 to 0.5
- gate_bias: float32 [128], replicated, may hold values from -3 to 3
- out_gain: float32 [128], replicated, may hold values from 0.1 to 1.9
- out_shift: float32 [128], replicated, may hold values from -3 to 3
- out_weight: bfloat16 [128, 128], replicated, may hold values from -0.5 to 0.5
- out_bias: float32 [128], replicated, may hold values from -3 to 3
Outputs:
- update: bfloat16 [768, 768, 128], P('row', 'col')
The draws below stay inside these ranges and needn't reach their ends.
All inputs are finite; a program needn't handle non-finite values.
Results may differ from the reference program's by a relative error of at most 0.0051.
Values may be sent and summed in bfloat16 or wider, within the bound.
A program may use at most 256 MiB of HBM per device.

```python
import jax
import jax.numpy as jnp
from jax import lax

C = 128
HID = 128
RES = 768


def block_levels(rng, dims, split, low, largest):
    level, own = 1.0, jax.random.fold_in(rng, 6)
    for position, blocks in split:
        heights = jnp.exp(jax.random.uniform(jax.random.fold_in(own, position), (blocks,), jnp.float32, low / len(split), largest / len(split)))
        level = level * jnp.repeat(heights, dims[position] // blocks).reshape([-1 if axis == position else 1 for axis in range(len(dims))])
    return level


def gaussian(key, shape, scale, limit, split=(), kind=jnp.bfloat16):
    result = scale * jax.random.normal(key, shape, jnp.float32)
    if split:
        result = result * block_levels(key, shape, split, -0.22, 0.18)
    return jnp.clip(result, -limit, limit).astype(kind)


def setup_inputs(seed: int = 0) -> dict:
    key_of = jax.random.split(jax.random.key(seed), 12)
    pair = gaussian(key_of[0], (RES, RES, C), 1.0, 6.0, ((0, 2), (1, 4)))
    ln_gain = jnp.clip(1.0 + 0.18 * jax.random.normal(key_of[1], (C,), jnp.float32), 0.1, 1.9)
    ln_shift = gaussian(key_of[2], (C,), 0.5, 3.0, (), jnp.float32)
    proj_weight = gaussian(key_of[3], (C, 4 * HID), C ** -0.5, 0.5)
    proj_bias = gaussian(key_of[4], (4 * HID,), 0.5, 3.0, (), jnp.float32)
    gate_weight = gaussian(key_of[5], (C, C), C ** -0.5, 0.5)
    gate_bias = gaussian(key_of[6], (C,), 0.5, 3.0, (), jnp.float32)
    out_gain = jnp.clip(1.0 + 0.18 * jax.random.normal(key_of[7], (HID,), jnp.float32), 0.1, 1.9)
    out_shift = gaussian(key_of[8], (HID,), 0.5, 3.0, (), jnp.float32)
    out_weight = gaussian(key_of[9], (HID, C), HID ** -0.5, 0.5)
    out_bias = gaussian(key_of[10], (C,), 0.5, 3.0, (), jnp.float32)
    return {"pair": pair, "ln_gain": ln_gain, "ln_shift": ln_shift, "proj_weight": proj_weight, "proj_bias": proj_bias, "gate_weight": gate_weight, "gate_bias": gate_bias, "out_gain": out_gain, "out_shift": out_shift, "out_weight": out_weight, "out_bias": out_bias}


def layer_norm(values, gain, shift):
    centre = lax.optimization_barrier(jnp.mean(values, axis=-1, keepdims=True))
    centred = values - centre
    spread = lax.optimization_barrier(jnp.mean(centred * centred, axis=-1, keepdims=True))
    return centred * lax.rsqrt(spread + 1e-05) * gain + shift

def reference(pair, ln_gain, ln_shift, proj_weight, proj_bias, gate_weight, gate_bias, out_gain, out_shift, out_weight, out_bias):
    hidden = proj_weight.shape[1] // 4
    normed = layer_norm(pair.astype(jnp.float32), ln_gain, ln_shift).astype(jnp.bfloat16)
    flat = normed.reshape(-1, C)
    mixed = jnp.dot(flat, proj_weight, preferred_element_type=jnp.float32) + proj_bias
    left = (jax.nn.sigmoid(mixed[:, :hidden]) * mixed[:, hidden:2 * hidden]).astype(jnp.bfloat16)
    right = (jax.nn.sigmoid(mixed[:, 2 * hidden:3 * hidden]) * mixed[:, 3 * hidden:]).astype(jnp.bfloat16)
    gate = jax.nn.sigmoid(jnp.dot(flat, gate_weight, preferred_element_type=jnp.float32) + gate_bias)
    left = left.reshape(RES, RES, hidden).astype(jnp.float32)
    right = right.reshape(RES, RES, hidden).astype(jnp.float32)
    triangle = jnp.einsum('ikc,jkc->ijc', left, right)
    tri_normed = layer_norm(triangle, out_gain, out_shift).astype(jnp.bfloat16)
    projected = jnp.dot(tri_normed.reshape(-1, hidden), out_weight, preferred_element_type=jnp.float32) + out_bias
    return (gate * projected).reshape(RES, RES, C).astype(jnp.bfloat16)
```

```python
import jax
import jax.numpy as jnp
from jax import lax
from jax.experimental import pallas as pl
from jax.experimental.pallas import tpu as pltpu
from jax.sharding import PartitionSpec as P

CHUNKS = 4


def layer_norm(values, gain, shift):
    centre = jnp.mean(values, axis=-1, keepdims=True)
    centred = values - centre
    spread = jnp.mean(centred * centred, axis=-1, keepdims=True)
    return centred * lax.rsqrt(spread + 1e-05) * gain + shift


def flipped_dot(a, b):
    return lax.dot_general(a, b, (((1,), (1,)), ((), ())), preferred_element_type=jnp.float32)


def project_kernel(x_ref, gain_ref, shift_ref, w_ref, b_ref, *refs):
    outs, (flat, made) = refs[:-2], refs[-2:]
    rows, step_k, channels = x_ref.shape
    count = w_ref.shape[0] // 4
    each = outs[0].shape[0]
    normed = layer_norm(x_ref[...].astype(jnp.float32), gain_ref[...], shift_ref[...])
    flat[...] = normed.reshape(rows * step_k, channels)
    lanes = made.shape[2]
    for k in range(step_k):
        line = flat[pl.ds(k, rows, stride=step_k), :].astype(jnp.bfloat16)
        mixed = flipped_dot(w_ref[...], line) + b_ref[...]
        left = jax.nn.sigmoid(mixed[:count]) * mixed[count : 2 * count]
        right = jax.nn.sigmoid(mixed[2 * count : 3 * count]) * mixed[3 * count :]
        for side, value in enumerate((left, right)):
            for tile in range(rows // lanes):
                made[tile, pl.ds(side * count * step_k + k, count, stride=step_k), :] = value[
                    :, tile * lanes : (tile + 1) * lanes
                ]
    for n, out in enumerate(outs):
        for tile in range(rows // lanes):
            size = each * step_k
            out[:, :, tile * lanes : (tile + 1) * lanes] = (
                made[tile, n * size : (n + 1) * size, :]
                .reshape(each, step_k, lanes)
                .astype(jnp.bfloat16)
            )


def project_all(pair, gain, shift, weight, bias, pieces, step_k):
    rows, cols, channels = pair.shape
    count = weight.shape[0] // 4
    each = count // pieces
    lanes = 128 if rows % 128 == 0 else rows
    whole = lambda *shape: pl.BlockSpec(shape, lambda k: (0,) * len(shape))
    return pl.pallas_call(
        project_kernel,
        grid=(cols // step_k,),
        in_specs=[
            pl.BlockSpec((rows, step_k, channels), lambda k: (0, k, 0)),
            whole(1, channels),
            whole(1, channels),
            whole(4 * count, channels),
            whole(4 * count, 1),
        ],
        out_specs=[pl.BlockSpec((each, step_k, rows), lambda k: (0, k, 0))] * (2 * pieces),
        out_shape=[jax.ShapeDtypeStruct((each, cols, rows), jnp.bfloat16)] * (2 * pieces),
        scratch_shapes=[
            pltpu.VMEM((rows * step_k, channels), jnp.float32),
            pltpu.VMEM((rows // lanes, 2 * count * step_k, lanes), jnp.float32),
        ],
        compiler_params=pltpu.CompilerParams(vmem_limit_bytes=60 * 1024 * 1024),
        cost_estimate=pl.CostEstimate(
            flops=2 * rows * cols * channels * 4 * count,
            bytes_accessed=4 * rows * cols * channels,
            transcendentals=rows * cols * 2 * count,
        ),
    )(pair, gain[None], shift[None], weight, bias[:, None])


def finish_kernel(x_ref, gain_ref, shift_ref, gw_ref, gb_ref, og_ref, os_ref, ow_ref, ob_ref, *refs):
    tris, (out, held, done) = refs[:-3], refs[-3:]
    rows, step_j, channels = x_ref.shape
    hidden = ow_ref.shape[0]
    tiles, lanes = held.shape[0], held.shape[2]
    each = tris[0].shape[0]
    for tile in range(tiles):
        cut = slice(tile * lanes, (tile + 1) * lanes)
        total = 0.0
        for tri in tris:
            total = total + jnp.sum(tri[:, :, cut].astype(jnp.float32), axis=0)
        centre = total / hidden
        spread = 0.0
        for tri in tris:
            centred = tri[:, :, cut].astype(jnp.float32) - centre[None]
            spread = spread + jnp.sum(centred * centred, axis=0)
        scale = lax.rsqrt(spread / hidden + 1e-05)
        for n, tri in enumerate(tris):
            centred = tri[:, :, cut].astype(jnp.float32) - centre[None]
            held[tile, n * each * step_j : (n + 1) * each * step_j, :] = (
                centred * scale[None]
            ).reshape(each * step_j, lanes)
    for j in range(step_j):
        for tile in range(tiles):
            value = held[tile, pl.ds(j, hidden, stride=step_j), :]
            value = (value * og_ref[...] + os_ref[...]).astype(jnp.bfloat16)
            projected = lax.dot_general(
                value, ow_ref[...], (((0,), (0,)), ((), ())), preferred_element_type=jnp.float32
            )
            done[pl.ds(tile * lanes * step_j + j, lanes, stride=step_j), :] = projected
    normed = layer_norm(x_ref[...].astype(jnp.float32), gain_ref[...], shift_ref[...])
    flat = normed.reshape(rows * step_j, channels).astype(jnp.bfloat16)
    gate = jax.nn.sigmoid(
        jnp.dot(flat, gw_ref[...], preferred_element_type=jnp.float32) + gb_ref[...]
    )
    update = gate * (done[...] + ob_ref[...])
    out[...] = update.reshape(rows, step_j, channels).astype(jnp.bfloat16)


def finish_all(pair, core, part, gain, shift, gw, gb, og, os, ow, ob, tris, step_j):
    rows, _, channels = pair.shape
    hidden = ow.shape[0]
    lanes = 128 if rows % 128 == 0 else rows
    each = tris[0].shape[0]
    here = lax.dynamic_slice_in_dim(pair, core * part, part, 1)
    whole = lambda *shape: pl.BlockSpec(shape, lambda j: (0,) * len(shape))
    return pl.pallas_call(
        finish_kernel,
        grid=(part // step_j,),
        in_specs=[
            pl.BlockSpec((rows, step_j, channels), lambda j: (0, j, 0)),
            whole(1, channels),
            whole(1, channels),
            whole(channels, channels),
            whole(1, channels),
            whole(hidden, 1),
            whole(hidden, 1),
            whole(hidden, channels),
            whole(1, channels),
        ]
        + [pl.BlockSpec((each, step_j, rows), lambda j: (0, j, 0))] * len(tris),
        out_specs=pl.BlockSpec((rows, step_j, channels), lambda j: (0, j, 0)),
        out_shape=jax.ShapeDtypeStruct((rows, part, channels), jnp.bfloat16),
        scratch_shapes=[
            pltpu.VMEM((rows // lanes, hidden * step_j, lanes), jnp.float32),
            pltpu.VMEM((rows * step_j, channels), jnp.float32),
        ],
        compiler_params=pltpu.CompilerParams(vmem_limit_bytes=60 * 1024 * 1024),
        cost_estimate=pl.CostEstimate(
            flops=4 * rows * part * channels * channels,
            bytes_accessed=6 * rows * part * channels,
            transcendentals=rows * part * channels,
        ),
    )(here, gain[None], shift[None], gw, gb[None], og[:, None], os[:, None], ow, ob[None], *tris)


def swap(value, axis, bit):
    count = lax.axis_size(axis)
    return lax.ppermute(value, axis, [(n, n ^ bit) for n in range(count)])


def pick(first_mine, mine, other):
    return jnp.where(first_mine, mine, other), jnp.where(first_mine, other, mine)


def cross_term(lefts, far, chunk, contract):
    left_far, (_, near), (_, beyond) = far[chunk]
    return (contract(near, lefts[chunk]) + contract(beyond, left_far)).astype(jnp.bfloat16)


def per_device(
    pair,
    ln_gain,
    ln_shift,
    proj_weight,
    proj_bias,
    gate_weight,
    gate_bias,
    out_gain,
    out_shift,
    out_weight,
    out_bias,
):
    rows_n, cols_n, depth_n = (lax.axis_size(a) for a in ("row", "col", "depth"))
    row, col, depth = (lax.axis_index(a) for a in ("row", "col", "depth"))
    rows, cols, channels = pair.shape
    hidden = proj_weight.shape[1] // 4
    low, high = col % 2, col // 2
    core = depth % 2
    per_depth = hidden // depth_n
    per_col = per_depth // 2
    step = per_col // CHUNKS
    half_j = 2 * cols
    part = cols // 2

    weight = proj_weight.T.reshape(4, hidden, channels)
    bias = proj_bias.reshape(4, hidden)
    first = depth * per_depth
    mine = lax.dynamic_slice_in_dim(weight, first, per_depth, 1)
    mine_bias = lax.dynamic_slice_in_dim(bias, first, per_depth, 1)
    mine = jnp.where(low == 0, mine, jnp.roll(mine, per_col, 1))
    mine_bias = jnp.where(low == 0, mine_bias, jnp.roll(mine_bias, per_col, 1))
    step_k = 16
    made = project_all(
        pair, ln_gain, ln_shift, mine.reshape(-1, channels), mine_bias.reshape(-1), 2 * CHUNKS, step_k
    )
    lefts, rights = made[: 2 * CHUNKS], made[2 * CHUNKS :]

    def gather_rows(right):
        if rows_n == 2:
            return pick(row == high, right, swap(right, "row", 1))
        whole = lax.all_gather(right, "row", axis=2, tiled=True)
        return (
            lax.dynamic_slice_in_dim(whole, high * half_j, half_j, 2),
            lax.dynamic_slice_in_dim(whole, (1 - high) * half_j, half_j, 2),
        )

    def contract(right, left):
        return jnp.einsum("hkj,hki->hji", right, left, preferred_element_type=jnp.float32)

    gathered = []
    far, crossed = [], []
    for chunk in range(CHUNKS):
        ahead = (lefts[CHUNKS + chunk], rights[CHUNKS + chunk])
        if chunk >= 2:
            *ahead, crossed[chunk - 2] = lax.optimization_barrier((*ahead, crossed[chunk - 2]))
        left_far, right_far = (swap(value, "col", 1) for value in ahead)
        far.append((left_far, gather_rows(rights[chunk]), gather_rows(right_far)))
        if chunk >= 1:
            crossed.append(cross_term(lefts, far, chunk - 1, contract))
    crossed.append(cross_term(lefts, far, CHUNKS - 1, contract))
    for chunk in range(CHUNKS):
        left_near = lefts[chunk]
        left_far, (near_own, _), (far_own, _) = far[chunk]
        arrived = swap(crossed[chunk], "col", 2)
        own = contract(near_own, left_near) + contract(far_own, left_far)
        triangle = (own + arrived.astype(jnp.float32)).astype(jnp.bfloat16)
        keep = lax.dynamic_slice_in_dim(triangle, low * cols, cols, 1)
        give = lax.dynamic_slice_in_dim(triangle, (1 - low) * cols, cols, 1)
        block = jnp.concatenate([keep, swap(give, "col", 1)], axis=0)
        same = lax.dynamic_slice_in_dim(block, core * part, part, 1)
        across = lax.dynamic_slice_in_dim(block, (1 - core) * part, part, 1)
        gathered += [
            same,
            swap(across, "depth", 1),
            swap(same, "depth", 2),
            swap(across, "depth", 3),
        ]

    order = jnp.concatenate(
        [
            (depth ^ m) * per_depth + (low ^ n) * per_col + chunk * step + jnp.arange(step)
            for chunk in range(CHUNKS)
            for m in range(4)
            for n in range(2)
        ]
    )
    finished = finish_all(
        pair,
        core,
        part,
        ln_gain,
        ln_shift,
        gate_weight,
        gate_bias,
        out_gain[order],
        out_shift[order],
        out_weight[order],
        out_bias,
        gathered,
        step_k,
    )
    first, second = pick(core == 0, finished, swap(finished, "depth", 1))
    return jnp.concatenate([first, second], axis=1)


def solution(mesh):
    placed = (P("row", "col", None), P(), P(), P(), P(), P(), P(), P(), P(), P(), P())
    return jax.shard_map(
        per_device, mesh=mesh, in_specs=placed, out_specs=P("row", "col", None), check_vma=False
    )
```
